32 devices in a mesh: section: 4 (over y, x), dp: 8 (over z, core).
Axes of the slice: x: 2, y: 2, z: 4, core: 2. Of those that a mesh axis runs over, the one named last changes fastest.
Arguments:
- token_ids: int32 [4, 512], P(None, 'dp'), may hold values from 0 to 127
- embed: bfloat16 [128, 512], replicated, may hold values from -6 to 6
- weights: bfloat16 [4, 2, 512, 2048], P('section'), may hold values from -0.25 to 0.25
- variance: bfloat16 [4, 1024, 2048], P('section', 'dp'), may hold values from 9.9658966e-05 to 0.0099487305
- momentum: bfloat16 [4, 1024, 2048], P('section', 'dp'), may hold values from -4 to 4
- worker_error: bfloat16 [4, 8, 2, 512, 2048], P('section', 'dp'), may hold values from -6 to 6
- server_error: float32 [4, 1024, 2048], P('section', 'dp'), may hold values from -0.75 to 0.75
- cotangent: bfloat16 [4, 512, 512], P(None, 'dp'), may hold values from -0.75 to 0.75
Outputs:
- new_weights: bfloat16 [4, 1024, 2048], P('section', 'dp')
- new_momentum: bfloat16 [4, 1024, 2048], P('section', 'dp')
- new_worker_error: bfloat16 [4, 8, 2, 512, 2048], P('section', 'dp')
- new_server_error: float32 [4, 1024, 2048], P('section', 'dp')
The draws below stay inside these ranges and needn't reach their ends.
All inputs are finite; a program needn't handle non-finite values.
Results may differ from the reference program's by a relative error of at most 0.012.
Values may be sent and summed in bfloat16 or wider, within the bound.
A program may use at most 128 MiB of HBM per device.

```python
import math
import jax
import jax.numpy as jnp
import numpy as np
from jax import lax

D = 512
HC = 2048
VW = 128
MB = 4
TOK_MB = 64
TOKENS = 512
N_SECTION = 4
N_DP = 8


def with_ends(entries, own_key, least, high):
    longest = entries.shape.index(max(entries.shape))
    spots = []
    for shift in (0, 1):
        where = [jax.random.randint(jax.random.fold_in(own_key, axis), (), 0, length) for axis, length in enumerate(entries.shape)]
        where[longest] = (where[longest] + shift) % entries.shape[longest]
        spots.append(tuple(where))
    return entries.at[spots[0]].set(least).at[spots[1]].set(high)


def with_spikes(values, stream_key, source, target, blocks, factor):
    owner, partner = [(jnp.arange(values.shape[dim]) // (values.shape[dim] // blocks)).reshape([-1 if axis == dim else 1 for axis in range(values.ndim)]) for dim in (source, target)]
    chosen = jax.random.permutation(stream_key, blocks)[partner]
    strong = (owner == chosen) | (owner == (partner + blocks // 2) % blocks)
    return jnp.where(strong, factor * values, values)


def block_scale(own_key, shape, shards, smallest, largest):
    level = 1.0
    for axis_at, parts in shards:
        draws = jax.random.uniform(jax.random.fold_in(jax.random.fold_in(own_key, 6), axis_at), (parts,), jnp.float32, smallest / len(shards), largest / len(shards))
        level = level * jnp.repeat(jnp.exp(draws), shape[axis_at] // parts).reshape((-1,) + (1,) * (len(shape) - 1 - axis_at))
    return level


def rank_table(number_of, slope):
    weights = [(1 << 20) // math.isqrt(standing ** slope) + 1 for standing in range(1, number_of + 1)]
    width = 1 + sum(weights) // (1 << 30)
    return np.cumsum(np.array([max(1, weight // width) for weight in weights]))


def skewed_ids(own_key, extent, count, slope):
    table = rank_table(count, slope)
    pick = jax.random.randint(jax.random.fold_in(own_key, 1), extent, 0, int(table[count - 1]))
    standing = jnp.searchsorted(jnp.asarray(table, jnp.int32), pick, side="right")
    return jax.random.permutation(jax.random.fold_in(own_key, 2), count)[standing].astype(jnp.int32)


def centred(key, shape, width, limit, shards=(), kind=jnp.bfloat16):
    values = width * jax.random.normal(key, shape, jnp.float32)
    if shards:
        values = values * block_scale(key, shape, shards, -0.22, 0.18)
    return jnp.clip(values, -limit, limit).astype(kind)


def heavy_noise(rng, dims, deviation, reach, shards, heavy, kind=jnp.bfloat16):
    result = deviation * jax.random.normal(rng, dims, jnp.float32)
    if shards:
        result = result * block_scale(rng, dims, shards, -0.22, 0.18)
    return jnp.clip(with_spikes(result, jax.random.fold_in(rng, 3), *heavy), -reach, reach).astype(kind)


def setup_inputs(seed: int = 0) -> dict:
    splits = jax.random.split(jax.random.key(seed), 9)
    token_ids = with_ends(skewed_ids(splits[0], (MB, TOKENS), VW, 2), jax.random.fold_in(splits[0], 3), 0, VW - 1).astype(jnp.int32)
    embed = centred(splits[1], (VW, D), 1.0, 6.0)
    weights = centred(splits[2], (N_SECTION, 2, D, HC), D ** -0.5, 0.25, ((0, 4),))
    variance = jnp.clip(jnp.exp(math.log(0.0099487305) - 4.603446 * jax.random.uniform(splits[3], (N_SECTION, 2 * D, HC), jnp.float32) ** block_scale(splits[3], (N_SECTION, 2 * D, HC), ((0, 4), (1, 8)), -0.2, 0.2)), 9.965896606445312e-05, 0.0099487305).astype(jnp.bfloat16)
    momentum = centred(splits[4], (N_SECTION, 2 * D, HC), 0.5, 4.0, ((0, 4), (1, 8)))
    worker_error = heavy_noise(splits[5], (N_SECTION, N_DP, 2, D, HC), 0.3, 6.0, ((0, 4), (1, 8)), (1, 3, 8, 2.0))
    server_error = centred(splits[6], (N_SECTION, 2 * D, HC), 0.05, 0.75, ((0, 4), (1, 8)), jnp.float32)
    cotangent = centred(splits[7], (MB, TOKENS, D), 0.05, 0.75, ((1, 8),))
    return dict(token_ids=token_ids, embed=embed, weights=weights, variance=variance, momentum=momentum, worker_error=worker_error, server_error=server_error, cotangent=cotangent)


gelu_coef = math.sqrt(2.0 / math.pi)

def gelu_value(upper):
    inner = gelu_coef * (upper + 0.044715 * upper * upper * upper)
    return 0.5 * upper * (1.0 + jnp.tanh(inner))

def gelu_slope(upper):
    inner = gelu_coef * (upper + 0.044715 * upper * upper * upper)
    bent = jnp.tanh(inner)
    return 0.5 * (1.0 + bent) + 0.5 * upper * (1.0 - bent * bent) * gelu_coef * (1.0 + 3.0 * 0.044715 * upper * upper)

def normalize(inputs):
    values = inputs.astype(jnp.float32)
    center = lax.optimization_barrier(jnp.mean(values, axis=-1, keepdims=True))
    spread = lax.optimization_barrier(jnp.mean((values - center) * (values - center), axis=-1, keepdims=True))
    scaled = lax.rsqrt(spread + 1e-05)
    return ((values - center) * scaled, scaled)

def forward_block(inputs, first_matrix, second_matrix):
    normed, scaled = normalize(inputs)
    normed_b = normed.astype(jnp.bfloat16)
    upper = jnp.dot(normed_b, first_matrix, preferred_element_type=jnp.float32)
    hidden = gelu_value(upper).astype(jnp.bfloat16)
    mixed = lax.dot_general(hidden, second_matrix, (((1,), (1,)), ((), ())), preferred_element_type=jnp.float32)
    output = (inputs.astype(jnp.float32) + mixed).astype(jnp.bfloat16)
    return (output, normed, scaled, normed_b, upper, hidden)

def backward_block(grad_out, normed, scaled, upper, first_matrix, second_matrix):
    back_hidden = jnp.dot(grad_out, second_matrix, preferred_element_type=jnp.float32)
    back_upper = (back_hidden * gelu_slope(upper)).astype(jnp.bfloat16)
    back_normed = lax.dot_general(back_upper, first_matrix, (((1,), (1,)), ((), ())), preferred_element_type=jnp.float32)
    first_mean = lax.optimization_barrier(jnp.mean(back_normed, axis=-1, keepdims=True))
    second_mean = lax.optimization_barrier(jnp.mean(back_normed * normed, axis=-1, keepdims=True))
    grad_in = (grad_out.astype(jnp.float32) + scaled * (back_normed - first_mean - normed * second_mean)).astype(jnp.bfloat16)
    return (grad_in, back_upper)

def replica_sum(left, right):
    left_rows = left.astype(jnp.float32).reshape(MB, N_DP, TOK_MB, left.shape[-1])
    right_rows = right.astype(jnp.float32).reshape(MB, N_DP, TOK_MB, right.shape[-1])
    return jnp.einsum('mrtd,mrth->rdh', left_rows, right_rows, precision=lax.Precision.HIGHEST)

def reference(token_ids, embed, weights, variance, momentum, worker_error, server_error, cotangent):
    state = jnp.take(embed, token_ids.reshape(-1).astype(jnp.int32), axis=0)
    saved = []
    for section in range(N_SECTION):
        output, normed, scaled, normed_b, upper, hidden = forward_block(state, weights[section, 0], weights[section, 1])
        saved.append((normed, scaled, normed_b, upper, hidden))
        state = output
    grad = cotangent.reshape(-1, D)
    results = [None] * N_SECTION
    for section in range(N_SECTION - 1, -1, -1):
        normed, scaled, normed_b, upper, hidden = saved[section]
        grad_in, back_upper = backward_block(grad, normed, scaled, upper, weights[section, 0], weights[section, 1])
        gradient = jnp.stack([replica_sum(normed_b, back_upper), replica_sum(grad, hidden)], axis=1)
        shared = momentum[section].astype(jnp.float32).reshape(2, D, HC)
        combined = 0.9 * shared[None] + 0.1 * gradient + worker_error[section].astype(jnp.float32)
        worker_scale = jnp.sqrt(lax.optimization_barrier(jnp.mean(combined * combined, axis=(1, 2, 3), keepdims=True)) + 0.01)
        packed = (worker_scale * jnp.tanh(combined / worker_scale)).astype(jnp.bfloat16)
        fresh_worker = (combined - packed.astype(jnp.float32)).astype(jnp.bfloat16)
        merged = (lax.optimization_barrier(jnp.sum(packed.astype(jnp.float32), axis=0)) / N_DP).reshape(2 * D, HC) + server_error[section]
        blocks = merged.reshape(N_DP, -1)
        server_scale = jnp.sqrt(lax.optimization_barrier(jnp.mean(blocks * blocks, axis=1, keepdims=True)) + 0.01)
        server_values = (server_scale * jnp.tanh(blocks / server_scale)).astype(jnp.bfloat16)
        fresh_server = (blocks - server_values.astype(jnp.float32)).reshape(2 * D, HC)
        averaged = server_values.reshape(2 * D, HC)
        step_size = 0.01 * averaged.astype(jnp.float32) / (jnp.sqrt(variance[section].astype(jnp.float32)) + 1e-08)
        fresh_weights = (weights[section].astype(jnp.float32).reshape(2 * D, HC) - step_size).astype(jnp.bfloat16)
        results[section] = (fresh_weights, averaged, fresh_worker, fresh_server)
        grad = grad_in
    new_weights = jnp.stack([item[0] for item in results])
    new_momentum = jnp.stack([item[1] for item in results])
    new_worker_error = jnp.stack([item[2] for item in results])
    new_server_error = jnp.stack([item[3] for item in results])
    return (new_weights, new_momentum, new_worker_error, new_server_error)
```

```python
import functools
import math

import jax
import jax.numpy as jnp
from jax import lax
from jax.experimental import pallas as pl
from jax.experimental.pallas import tpu as pltpu
from jax.sharding import PartitionSpec as P

gelu_coef = math.sqrt(2.0 / math.pi)
MESH = pl.DeviceIdType.MESH
NT = (((1,), (1,)), ((), ()))
TN = (((0,), (0,)), ((), ()))


def dot(left, right, dims=(((1,), (0,)), ((), ()))):
    return lax.dot_general(left, right, dims, preferred_element_type=jnp.float32)


def dp_device(index):
    return {"section": lax.axis_index("section"), "dp": index}


def section_device(index):
    return {"section": index, "dp": lax.axis_index("dp")}


def signal(semaphore, device):
    pl.semaphore_signal(semaphore, inc=1, device_id=device, device_id_type=MESH)


def remote(src, dst, send, recv, device):
    return pltpu.make_async_remote_copy(
        src_ref=src, dst_ref=dst, send_sem=send, recv_sem=recv, device_id=device, device_id_type=MESH
    )


def block_kernel(
    sections, chips, ids, embed, weights, cotangent, momentum, left, right, shared,
    arrived, outgoing, back_arrived, back_outgoing, normed_s, scaled_s, slope_s,
    fwd_send, fwd_recv, bwd_send, bwd_recv, own_sem, far_send, far_recv, pair_send, pair_recv,
):
    micro, rows, width = cotangent.shape
    vocab = embed.shape[0]
    channels = weights.shape[-1]
    tile = min(512, channels)
    owned = momentum.shape[0]
    section = lax.axis_index("section")
    me = lax.axis_index("dp")
    chip, core = me // 2, me % 2
    partner = chip * 2 + 1 - core
    first, last = section == 0, section == sections - 1
    ahead, behind = lax.rem(section + 1, sections), lax.rem(section + sections - 1, sections)

    barrier = pltpu.get_barrier_semaphore()
    signal(barrier, section_device(ahead))
    signal(barrier, section_device(behind))
    signal(barrier, dp_device(partner))
    for j in range(1, chips):
        signal(barrier, dp_device(lax.rem(chip + j, chips) * 2 + core))
    pl.semaphore_wait(barrier, 2 + chips)

    def span(index):
        return pl.ds(pl.multiple_of(index * owned, owned), owned)

    own_copy = pltpu.make_async_copy(momentum, shared.at[span(me)], own_sem)
    own_copy.start()
    far = []
    for j in range(1, chips):
        target = lax.rem(chip + j, chips) * 2 + core
        far.append(remote(momentum, shared.at[span(me)], far_send.at[j], far_recv.at[j], dp_device(target)))
        far[-1].start()
    pair = [remote(momentum, shared.at[span(me)], pair_send.at[0], pair_recv.at[0], dp_device(partner))]
    pair[0].start()

    def fwd_copy(m):
        return remote(outgoing.at[m], arrived.at[m], fwd_send.at[m], fwd_recv.at[m], section_device(ahead))

    def bwd_copy(m):
        return remote(
            back_outgoing.at[m], back_arrived.at[m], bwd_send.at[m], bwd_recv.at[m], section_device(behind)
        )

    @pl.when(first)
    def _():
        for m in range(micro):
            hot = ids[m : m + 1, :] == lax.broadcasted_iota(jnp.int32, (vocab, rows), 0)
            hot = jnp.where(hot, 1.0, 0.0).astype(jnp.bfloat16)
            arrived[m] = dot(hot, embed[...], TN).astype(jnp.bfloat16)

    def forward(m, carry):
        @pl.when(jnp.logical_not(first))
        def _():
            fwd_copy(m).wait_recv()

        values = arrived[m].astype(jnp.float32)
        center = jnp.mean(values, axis=-1, keepdims=True)
        shifted = values - center
        spread = jnp.mean(shifted * shifted, axis=-1, keepdims=True)
        scaled = lax.rsqrt(spread + 1e-05)
        normed = shifted * scaled
        normed_b = normed.astype(jnp.bfloat16)
        normed_s[m] = normed
        scaled_s[m] = scaled
        left[0, m] = normed_b
        mixed = values
        for start in range(0, channels, tile):
            cut = slice(start, start + tile)
            upper = dot(normed_b, weights[0, 0, :, cut])
            square = upper * upper
            bent = jnp.tanh(gelu_coef * (upper + 0.044715 * upper * square))
            half = 0.5 * (1.0 + bent)
            hidden = (upper * half).astype(jnp.bfloat16)
            right[1, m, :, cut] = hidden
            slope_s[m, :, cut] = half + 0.5 * upper * (1.0 - bent * bent) * gelu_coef * (
                1.0 + 3.0 * 0.044715 * square
            )
            mixed = mixed + dot(hidden, weights[0, 1, :, cut], NT)
        outgoing[m] = mixed.astype(jnp.bfloat16)

        @pl.when(jnp.logical_not(last))
        def _():
            fwd_copy(m).start()

        return carry

    lax.fori_loop(0, micro, forward, 0)

    def backward(m, carry):
        @pl.when(last)
        def _():
            left[1, m] = cotangent[m]

        @pl.when(jnp.logical_not(last))
        def _():
            bwd_copy(m).wait_recv()
            left[1, m] = back_arrived[m]

        grad_out = left[1, m]
        back_normed = jnp.zeros((rows, width), jnp.float32)
        for start in range(0, channels, tile):
            cut = slice(start, start + tile)
            back_hidden = dot(grad_out, weights[0, 1, :, cut])
            back_upper = (back_hidden * slope_s[m, :, cut]).astype(jnp.bfloat16)
            right[0, m, :, cut] = back_upper
            back_normed = back_normed + dot(back_upper, weights[0, 0, :, cut], NT)

        @pl.when(jnp.logical_not(first))
        def _():
            normed = normed_s[m]
            first_mean = jnp.mean(back_normed, axis=-1, keepdims=True)
            second_mean = jnp.mean(back_normed * normed, axis=-1, keepdims=True)
            back_outgoing[m] = (
                grad_out.astype(jnp.float32) + scaled_s[m] * (back_normed - first_mean - normed * second_mean)
            ).astype(jnp.bfloat16)
            bwd_copy(m).start()

        return carry

    lax.fori_loop(0, micro, backward, 0)

    own_copy.wait()
    for j in range(1, chips):
        far[j - 1].wait()
        origin = span(lax.rem(chip + chips - j, chips) * 2 + core)
        pair.append(
            remote(shared.at[origin], shared.at[origin], pair_send.at[j], pair_recv.at[j], dp_device(partner))
        )
        pair[-1].start()
    for copy in pair:
        copy.wait()

    @pl.when(jnp.logical_not(last))
    def _():
        for m in range(micro):
            fwd_copy(m).wait_send()

    @pl.when(jnp.logical_not(first))
    def _():
        for m in range(micro):
            bwd_copy(m).wait_send()


def run_blocks(sections, chips, ids, embed, weights, cotangent, momentum):
    micro, rows, width = cotangent.shape
    channels = weights.shape[-1]
    vmem = pl.BlockSpec(memory_space=pltpu.VMEM)
    hbm = pl.BlockSpec(memory_space=pl.ANY)
    relay = pltpu.VMEM((micro, rows, width), jnp.bfloat16)
    dma = pltpu.SemaphoreType.DMA
    return pl.pallas_call(
        functools.partial(block_kernel, sections, chips),
        out_shape=(
            jax.ShapeDtypeStruct((2, micro, rows, width), jnp.bfloat16),
            jax.ShapeDtypeStruct((2, micro, rows, channels), jnp.bfloat16),
            jax.ShapeDtypeStruct((2 * width, channels), jnp.bfloat16),
        ),
        in_specs=[vmem, vmem, vmem, vmem, hbm],
        out_specs=(vmem, vmem, hbm),
        scratch_shapes=[
            relay, relay, relay, relay,
            pltpu.VMEM((micro, rows, width), jnp.float32),
            pltpu.VMEM((micro, rows, 1), jnp.float32),
            pltpu.VMEM((micro, rows, channels), jnp.float32),
            dma((micro,)), dma((micro,)), dma((micro,)), dma((micro,)),
            dma, dma((chips,)), dma((chips,)), dma((chips,)), dma((chips,)),
        ],
        compiler_params=pltpu.CompilerParams(
            collective_id=0, has_side_effects=True, vmem_limit_bytes=48 * 1024 * 1024
        ),
        name="blocks",
    )(ids, embed, weights, cotangent, momentum)


def pack_kernel(count, left, right, shared, error, packed, fresh, combined, total):
    phase, step = pl.program_id(0), pl.program_id(1)

    @pl.when(jnp.logical_and(phase == 0, step == 0))
    def _():
        total[...] = jnp.zeros_like(total)

    @pl.when(phase == 0)
    def _():
        gradient = dot(left[0], right[0], TN)
        values = 0.9 * shared[...].astype(jnp.float32) + 0.1 * gradient + error[...].astype(jnp.float32)
        combined[step] = values
        total[...] += jnp.sum(values * values, axis=0, keepdims=True)

    @pl.when(phase == 1)
    def _():
        mean = jnp.sum(total[...], axis=1, keepdims=True) / count
        scale = jnp.sqrt(mean + 0.01)
        values = combined[step]
        narrow = (scale * jnp.tanh(values * (1.0 / scale))).astype(jnp.bfloat16)
        packed[...] = narrow
        fresh[...] = (values - narrow.astype(jnp.float32)).astype(jnp.bfloat16)


def pack(left, right, shared, error):
    _, tokens, width = left.shape
    channels = right.shape[-1]
    tile = 128
    per = width // tile
    steps = 2 * per

    def when_first(phase, step):
        return jnp.where(phase == 0, step, steps - 1)

    rows_in = pl.BlockSpec((tile, channels), lambda p, i: (when_first(p, i), 0))
    rows_out = pl.BlockSpec((tile, channels), lambda p, i: (jnp.where(p == 0, 0, i), 0))
    out = jax.ShapeDtypeStruct((2 * width, channels), jnp.bfloat16)
    return pl.pallas_call(
        functools.partial(pack_kernel, float(2 * width * channels)),
        grid=(2, steps),
        out_shape=(out, out),
        in_specs=[
            pl.BlockSpec((1, tokens, tile), lambda p, i: (when_first(p, i) // per, 0, when_first(p, i) % per)),
            pl.BlockSpec((1, tokens, channels), lambda p, i: (when_first(p, i) // per, 0, 0)),
            rows_in,
            rows_in,
        ],
        out_specs=(rows_out, rows_out),
        scratch_shapes=[
            pltpu.VMEM((steps, tile, channels), jnp.float32),
            pltpu.VMEM((1, channels), jnp.float32),
        ],
        compiler_params=pltpu.CompilerParams(
            dimension_semantics=("arbitrary", "arbitrary"), vmem_limit_bytes=48 * 1024 * 1024
        ),
        name="pack",
    )(left, right, shared, error)


def merge_kernel(
    chips, packed, total, own, paired, outgoing, arrived,
    own_sem, pair_send, pair_recv, far_send, far_recv,
):
    owned = total.shape[0]
    me = lax.axis_index("dp")
    chip, core = me // 2, me % 2
    other = 1 - core
    partner = chip * 2 + other

    barrier = pltpu.get_barrier_semaphore()
    signal(barrier, dp_device(partner))
    for j in range(1, chips):
        signal(barrier, dp_device(lax.rem(chip + j, chips) * 2 + core))
    pl.semaphore_wait(barrier, chips)

    def span(index):
        return pl.ds(pl.multiple_of(index * owned, owned), owned)

    order = list(range(1, chips)) + [0]
    local, pair, far = {}, {}, {}
    for j in order:
        target = lax.rem(chip + j, chips) * 2
        pair[j] = remote(
            packed.at[span(target + other)], paired.at[j], pair_send.at[j], pair_recv.at[j], dp_device(partner)
        )
        pair[j].start()
        local[j] = pltpu.make_async_copy(packed.at[span(target + core)], own.at[j], own_sem.at[j])
        local[j].start()
    for j in order:
        local[j].wait()
        pair[j].wait()
        both = own[j].astype(jnp.float32) + paired[j].astype(jnp.float32)
        if j == 0:
            total[...] = both
        else:
            outgoing[j - 1] = both.astype(jnp.bfloat16)
            target = lax.rem(chip + j, chips) * 2 + core
            far[j] = remote(
                outgoing.at[j - 1], arrived.at[j - 1], far_send.at[j], far_recv.at[j], dp_device(target)
            )
            far[j].start()
    for j in range(1, chips):
        far[j].wait()
        total[...] += arrived[j - 1].astype(jnp.float32)


def merge(chips, packed):
    rows, channels = packed.shape
    owned = rows // (2 * chips)
    dma = pltpu.SemaphoreType.DMA
    return pl.pallas_call(
        functools.partial(merge_kernel, chips),
        out_shape=jax.ShapeDtypeStruct((owned, channels), jnp.float32),
        in_specs=[pl.BlockSpec(memory_space=pl.ANY)],
        out_specs=pl.BlockSpec(memory_space=pltpu.VMEM),
        scratch_shapes=[
            pltpu.VMEM((chips, owned, channels), jnp.bfloat16),
            pltpu.VMEM((chips, owned, channels), jnp.bfloat16),
            pltpu.VMEM((chips - 1, owned, channels), jnp.bfloat16),
            pltpu.VMEM((chips - 1, owned, channels), jnp.bfloat16),
            dma((chips,)), dma((chips,)), dma((chips,)), dma((chips,)), dma((chips,)),
        ],
        compiler_params=pltpu.CompilerParams(
            collective_id=1, has_side_effects=True, vmem_limit_bytes=48 * 1024 * 1024
        ),
        name="merge",
    )(packed)


def local(sections, replicas, token_ids, embed, weights, variance, momentum, worker_error, server_error, cotangent):
    width, channels = weights.shape[2:]
    owned = 2 * width // replicas
    chips = replicas // 2
    left, right, shared = run_blocks(sections, chips, token_ids, embed, weights, cotangent, momentum[0])
    packed, new_worker = pack(
        left.reshape(2, -1, width),
        right.reshape(2, -1, channels),
        shared,
        worker_error.reshape(2 * width, channels),
    )
    total = merge(chips, packed)
    merged = total / replicas + server_error[0]
    server_scale = jnp.sqrt(jnp.mean(merged * merged) + 0.01)
    server_values = (server_scale * jnp.tanh(merged / server_scale)).astype(jnp.bfloat16)
    new_server = (merged - server_values.astype(jnp.float32))[None]
    start = lax.axis_index("dp") * owned
    own_weights = lax.dynamic_slice_in_dim(weights[0].reshape(2 * width, channels), start, owned, 0)
    step_size = (
        0.01 * server_values.astype(jnp.float32) / (jnp.sqrt(variance[0].astype(jnp.float32)) + 1e-08)
    )
    new_weights = (own_weights.astype(jnp.float32) - step_size).astype(jnp.bfloat16)[None]
    return (new_weights, server_values[None], new_worker.reshape(worker_error.shape), new_server)


def solution(mesh):
    in_specs = (
        P(None, "dp"),
        P(),
        P("section", None, None, None),
        P("section", "dp", None),
        P("section", "dp", None),
        P("section", "dp", None, None, None),
        P("section", "dp", None),
        P(None, "dp", None),
    )
    out_specs = (
        P("section", "dp", None),
        P("section", "dp", None),
        P("section", "dp", None, None, None),
        P("section", "dp", None),
    )
    body = functools.partial(local, mesh.shape["section"], mesh.shape["dp"])
    return jax.shard_map(body, mesh=mesh, in_specs=in_specs, out_specs=out_specs, check_vma=False)
```

```python
import functools
import math

import jax
import jax.numpy as jnp
from jax import lax
from jax.experimental import pallas as pl
from jax.experimental.pallas import tpu as pltpu
from jax.sharding import PartitionSpec as P

gelu_coef = math.sqrt(2.0 / math.pi)
MESH = pl.DeviceIdType.MESH
NT = (((1,), (1,)), ((), ()))
TN = (((0,), (0,)), ((), ()))


def dot(left, right, dims=(((1,), (0,)), ((), ()))):
    return lax.dot_general(left, right, dims, preferred_element_type=jnp.float32)


def dp_device(index):
    return {"section": lax.axis_index("section"), "dp": index}


def section_device(index):
    return {"section": index, "dp": lax.axis_index("dp")}


def signal(semaphore, device):
    pl.semaphore_signal(semaphore, inc=1, device_id=device, device_id_type=MESH)


def remote(src, dst, send, recv, device):
    return pltpu.make_async_remote_copy(
        src_ref=src, dst_ref=dst, send_sem=send, recv_sem=recv, device_id=device, device_id_type=MESH
    )


def block_kernel(
    sections, chips, ids, embed_in, weights_in, cotangent_in, momentum, left, right, shared,
    embed, first_matrix, second_matrix, cotangent, load_sem, arrived, outgoing, back_arrived, back_outgoing, normed_s, scaled_s, slope_s,
    fwd_send, fwd_recv, bwd_send, bwd_recv, own_sem, up_send, up_recv, down_send, down_recv, pair_send, pair_recv,
):
    micro, rows, width = cotangent.shape
    vocab = embed.shape[0]
    channels = first_matrix.shape[-1]
    loads = [
        pltpu.make_async_copy(embed_in, embed, load_sem.at[0]),
        pltpu.make_async_copy(weights_in.at[0, 0], first_matrix, load_sem.at[1]),
        pltpu.make_async_copy(weights_in.at[0, 1], second_matrix, load_sem.at[2]),
        pltpu.make_async_copy(cotangent_in, cotangent, load_sem.at[3]),
    ]
    for load in loads:
        load.start()
    tile = min(512, channels)
    owned = momentum.shape[0]
    section = lax.axis_index("section")
    me = lax.axis_index("dp")
    chip, core = me // 2, me % 2
    partner = chip * 2 + 1 - core
    first, last = section == 0, section == sections - 1
    ahead, behind = lax.rem(section + 1, sections), lax.rem(section + sections - 1, sections)

    barrier = pltpu.get_barrier_semaphore()
    signal(barrier, section_device(ahead))
    signal(barrier, section_device(behind))
    signal(barrier, dp_device(partner))
    for j in range(1, chips):
        signal(barrier, dp_device(lax.rem(chip + j, chips) * 2 + core))
    pl.semaphore_wait(barrier, 2 + chips)

    def span(index):
        return pl.ds(pl.multiple_of(index * owned, owned), owned)

    own_copy = pltpu.make_async_copy(momentum, shared.at[span(me)], own_sem)
    own_copy.start()

    def up_copy(hop):
        rows_of = span(me - 2 * hop)
        source = momentum if hop == 0 else shared.at[rows_of]
        return remote(source, shared.at[rows_of], up_send.at[hop], up_recv.at[hop], dp_device(me + 2))

    def down_copy(hop):
        rows_of = span(me + 2 * hop)
        source = momentum if hop == 0 else shared.at[rows_of]
        return remote(source, shared.at[rows_of], down_send.at[hop], down_recv.at[hop], dp_device(me - 2))

    def pair_copy(slot, index):
        source = momentum if slot == 0 else shared.at[span(index)]
        return remote(source, shared.at[span(index)], pair_send.at[slot], pair_recv.at[slot], dp_device(partner))

    def pass_on(hop):
        if hop > 0:
            @pl.when(chip >= hop)
            def _():
                up_copy(hop - 1).wait_recv()

        @pl.when(jnp.logical_and(chip >= hop, chip < chips - 1))
        def _():
            up_copy(hop).start()

        if hop > 0:
            @pl.when(chip + hop < chips)
            def _():
                down_copy(hop - 1).wait_recv()

        @pl.when(jnp.logical_and(chip + hop < chips, chip > 0))
        def _():
            down_copy(hop).start()

        if hop == 0:
            pair_copy(0, me).start()
        else:
            @pl.when(chip >= hop)
            def _():
                pair_copy(2 * hop - 1, me - 2 * hop).start()

            @pl.when(chip + hop < chips)
            def _():
                pair_copy(2 * hop, me + 2 * hop).start()

    pass_on(0)

    def fwd_copy(m):
        return remote(outgoing.at[m], arrived.at[m], fwd_send.at[m], fwd_recv.at[m], section_device(ahead))

    def bwd_copy(m):
        return remote(
            back_outgoing.at[m], back_arrived.at[m], bwd_send.at[m], bwd_recv.at[m], section_device(behind)
        )

    loads[0].wait()

    @pl.when(first)
    def _():
        for m in range(micro):
            hot = ids[m : m + 1, :] == lax.broadcasted_iota(jnp.int32, (vocab, rows), 0)
            hot = jnp.where(hot, 1.0, 0.0).astype(jnp.bfloat16)
            arrived[m] = dot(hot, embed[...], TN).astype(jnp.bfloat16)

    loads[1].wait()
    loads[2].wait()
    if chips > 2:
        @pl.when(last)
        def _():
            pass_on(1)

    def forward(m, carry):
        @pl.when(jnp.logical_not(first))
        def _():
            fwd_copy(m).wait_recv()

        values = arrived[m].astype(jnp.float32)
        center = jnp.mean(values, axis=-1, keepdims=True)
        shifted = values - center
        spread = jnp.mean(shifted * shifted, axis=-1, keepdims=True)
        scaled = lax.rsqrt(spread + 1e-05)
        normed = shifted * scaled
        normed_b = normed.astype(jnp.bfloat16)
        normed_s[m] = normed
        scaled_s[m] = scaled
        left[0, m] = normed_b
        mixed = values
        for start in range(0, channels, tile):
            cut = slice(start, start + tile)
            upper = dot(normed_b, first_matrix[:, cut])
            square = upper * upper
            bent = jnp.tanh(gelu_coef * (upper + 0.044715 * upper * square))
            half = 0.5 * (1.0 + bent)
            hidden = (upper * half).astype(jnp.bfloat16)
            right[1, m, :, cut] = hidden
            slope_s[m, :, cut] = half + 0.5 * upper * (1.0 - bent * bent) * gelu_coef * (
                1.0 + 3.0 * 0.044715 * square
            )
            mixed = mixed + dot(hidden, second_matrix[:, cut], NT)
        outgoing[m] = mixed.astype(jnp.bfloat16)

        @pl.when(jnp.logical_not(last))
        def _():
            fwd_copy(m).start()

        return carry

    lax.fori_loop(0, micro, forward, 0)
    loads[3].wait()

    @pl.when(jnp.logical_not(last))
    def _():
        for hop in range(1, chips - 1):
            pass_on(hop)

    def backward(m, carry):
        @pl.when(last)
        def _():
            left[1, m] = cotangent[m]

        @pl.when(jnp.logical_not(last))
        def _():
            bwd_copy(m).wait_recv()
            left[1, m] = back_arrived[m]

        grad_out = left[1, m]
        back_normed = jnp.zeros((rows, width), jnp.float32)
        for start in range(0, channels, tile):
            cut = slice(start, start + tile)
            back_hidden = dot(grad_out, second_matrix[:, cut])
            back_upper = (back_hidden * slope_s[m, :, cut]).astype(jnp.bfloat16)
            right[0, m, :, cut] = back_upper
            back_normed = back_normed + dot(back_upper, first_matrix[:, cut], NT)

        @pl.when(jnp.logical_not(first))
        def _():
            normed = normed_s[m]
            first_mean = jnp.mean(back_normed, axis=-1, keepdims=True)
            second_mean = jnp.mean(back_normed * normed, axis=-1, keepdims=True)
            back_outgoing[m] = (
                grad_out.astype(jnp.float32) + scaled_s[m] * (back_normed - first_mean - normed * second_mean)
            ).astype(jnp.bfloat16)
            bwd_copy(m).start()

        return carry

    lax.fori_loop(0, micro, backward, 0)

    @pl.when(last)
    def _():
        for hop in range(2, chips - 1):
            pass_on(hop)

    pass_on(chips - 1)
    own_copy.wait()
    pair_copy(0, me).wait()
    for hop in range(chips):
        @pl.when(jnp.logical_and(chip >= hop, chip < chips - 1))
        def _():
            up_copy(hop).wait_send()

        @pl.when(jnp.logical_and(chip + hop < chips, chip > 0))
        def _():
            down_copy(hop).wait_send()

        if hop > 0:
            @pl.when(chip >= hop)
            def _():
                pair_copy(2 * hop - 1, me - 2 * hop).wait()

            @pl.when(chip + hop < chips)
            def _():
                pair_copy(2 * hop, me + 2 * hop).wait()

    @pl.when(jnp.logical_not(last))
    def _():
        for m in range(micro):
            fwd_copy(m).wait_send()

    @pl.when(jnp.logical_not(first))
    def _():
        for m in range(micro):
            bwd_copy(m).wait_send()


def run_blocks(sections, chips, ids, embed, weights, cotangent, momentum):
    micro, rows, width = cotangent.shape
    channels = weights.shape[-1]
    vmem = pl.BlockSpec(memory_space=pltpu.VMEM)
    hbm = pl.BlockSpec(memory_space=pl.ANY)
    relay = pltpu.VMEM((micro, rows, width), jnp.bfloat16)
    dma = pltpu.SemaphoreType.DMA
    return pl.pallas_call(
        functools.partial(block_kernel, sections, chips),
        out_shape=(
            jax.ShapeDtypeStruct((2, micro, rows, width), jnp.bfloat16),
            jax.ShapeDtypeStruct((2, micro, rows, channels), jnp.bfloat16),
            jax.ShapeDtypeStruct((2 * width, channels), jnp.bfloat16),
        ),
        in_specs=[vmem, hbm, hbm, hbm, hbm],
        out_specs=(vmem, vmem, hbm),
        scratch_shapes=[
            pltpu.VMEM(embed.shape, jnp.bfloat16),
            pltpu.VMEM((width, channels), jnp.bfloat16),
            pltpu.VMEM((width, channels), jnp.bfloat16),
            relay, dma((4,)), relay, relay, relay, relay,
            pltpu.VMEM((micro, rows, width), jnp.float32),
            pltpu.VMEM((micro, rows, 1), jnp.float32),
            pltpu.VMEM((micro, rows, channels), jnp.float32),
            dma((micro,)), dma((micro,)), dma((micro,)), dma((micro,)),
            dma, dma((chips,)), dma((chips,)), dma((chips,)), dma((chips,)),
            dma((2 * chips,)), dma((2 * chips,)),
        ],
        compiler_params=pltpu.CompilerParams(
            collective_id=0, has_side_effects=True, vmem_limit_bytes=60 * 1024 * 1024
        ),
        name="blocks",
    )(ids, embed, weights, cotangent, momentum)


def pack_kernel(count, left, right, shared, error, packed, fresh, combined, total):
    phase, step = pl.program_id(0), pl.program_id(1)

    @pl.when(jnp.logical_and(phase == 0, step == 0))
    def _():
        total[...] = jnp.zeros_like(total)

    @pl.when(phase == 0)
    def _():
        gradient = dot(left[0], right[0], TN)
        values = 0.9 * shared[...].astype(jnp.float32) + 0.1 * gradient + error[...].astype(jnp.float32)
        combined[step] = values
        total[...] += jnp.sum(values * values, axis=0, keepdims=True)

    @pl.when(phase == 1)
    def _():
        mean = jnp.sum(total[...], axis=1, keepdims=True) / count
        scale = jnp.sqrt(mean + 0.01)
        values = combined[step]
        narrow = (scale * jnp.tanh(values * (1.0 / scale))).astype(jnp.bfloat16)
        packed[...] = narrow
        fresh[...] = (values - narrow.astype(jnp.float32)).astype(jnp.bfloat16)


def pack(left, right, shared, error):
    _, tokens, width = left.shape
    channels = right.shape[-1]
    tile = 128
    per = width // tile
    steps = 2 * per

    def when_first(phase, step):
        return jnp.where(phase == 0, step, steps - 1)

    rows_in = pl.BlockSpec((tile, channels), lambda p, i: (when_first(p, i), 0))
    rows_out = pl.BlockSpec((tile, channels), lambda p, i: (jnp.where(p == 0, 0, i), 0))
    out = jax.ShapeDtypeStruct((2 * width, channels), jnp.bfloat16)
    return pl.pallas_call(
        functools.partial(pack_kernel, float(2 * width * channels)),
        grid=(2, steps),
        out_shape=(out, out),
        in_specs=[
            pl.BlockSpec((1, tokens, tile), lambda p, i: (when_first(p, i) // per, 0, when_first(p, i) % per)),
            pl.BlockSpec((1, tokens, channels), lambda p, i: (when_first(p, i) // per, 0, 0)),
            rows_in,
            rows_in,
        ],
        out_specs=(rows_out, rows_out),
        scratch_shapes=[
            pltpu.VMEM((steps, tile, channels), jnp.float32),
            pltpu.VMEM((1, channels), jnp.float32),
        ],
        compiler_params=pltpu.CompilerParams(
            dimension_semantics=("arbitrary", "arbitrary"), vmem_limit_bytes=60 * 1024 * 1024
        ),
        name="pack",
    )(left, right, shared, error)


def merge_kernel(
    chips, packed, total, own, paired, outgoing, arrived,
    own_sem, pair_send, pair_recv, far_send, far_recv,
):
    owned = total.shape[0]
    me = lax.axis_index("dp")
    chip, core = me // 2, me % 2
    other = 1 - core
    partner = chip * 2 + other

    barrier = pltpu.get_barrier_semaphore()
    signal(barrier, dp_device(partner))
    for j in range(1, chips):
        signal(barrier, dp_device(lax.rem(chip + j, chips) * 2 + core))
    pl.semaphore_wait(barrier, chips)

    def span(index):
        return pl.ds(pl.multiple_of(index * owned, owned), owned)

    order = list(range(1, chips)) + [0]
    local, pair, far = {}, {}, {}
    for j in order:
        target = lax.rem(chip + j, chips) * 2
        pair[j] = remote(
            packed.at[span(target + other)], paired.at[j], pair_send.at[j], pair_recv.at[j], dp_device(partner)
        )
        pair[j].start()
        local[j] = pltpu.make_async_copy(packed.at[span(target + core)], own.at[j], own_sem.at[j])
        local[j].start()
    for j in order:
        local[j].wait()
        pair[j].wait()
        both = own[j].astype(jnp.float32) + paired[j].astype(jnp.float32)
        if j == 0:
            total[...] = both
        else:
            outgoing[j - 1] = both.astype(jnp.bfloat16)
            target = lax.rem(chip + j, chips) * 2 + core
            far[j] = remote(
                outgoing.at[j - 1], arrived.at[j - 1], far_send.at[j], far_recv.at[j], dp_device(target)
            )
            far[j].start()
    for j in range(1, chips):
        far[j].wait()
        total[...] += arrived[j - 1].astype(jnp.float32)


def line_kernel(
    chips, packed, total, own, paired, up_out, up_in, down_out, down_in,
    own_sem, pair_send, pair_recv, up_send, up_recv, down_send, down_recv,
):
    owned = total.shape[0]
    me = lax.axis_index("dp")
    chip, core = me // 2, me % 2
    other = 1 - core
    partner = chip * 2 + other

    barrier = pltpu.get_barrier_semaphore()
    signal(barrier, dp_device(partner))
    for j in range(1, chips):
        signal(barrier, dp_device(lax.rem(chip + j, chips) * 2 + core))
    pl.semaphore_wait(barrier, chips)

    def span(index):
        return pl.ds(pl.multiple_of(index * owned, owned), owned)

    def up_copy(to):
        return remote(up_out.at[to], up_in.at[to], up_send.at[to], up_recv.at[to], dp_device(me + 2))

    def down_copy(to):
        return remote(down_out.at[to], down_in.at[to], down_send.at[to], down_recv.at[to], dp_device(me - 2))

    def at_chip(here):
        work = [(here + chips - 1 - to, to, 0) for to in range(here, chips) if to > here or here > 0]
        work += [(chips - 1 - here + to, to, 1) for to in range(here + 1) if to < here or here < chips - 1]
        work.sort()
        order = []
        for _, to, _ in work:
            if to != here and to not in order:
                order.append(to)
        order.append(here)
        local, pair, done, started = {}, {}, set(), []
        for to in order:
            pair[to] = remote(
                packed.at[span(2 * to + other)], paired.at[to], pair_send.at[to], pair_recv.at[to], dp_device(partner)
            )
            pair[to].start()
            local[to] = pltpu.make_async_copy(packed.at[span(2 * to + core)], own.at[to], own_sem.at[to])
            local[to].start()

        def both(to):
            if to not in done:
                done.add(to)
                local[to].wait()
                pair[to].wait()
            return own[to].astype(jnp.float32) + paired[to].astype(jnp.float32)

        filled = False
        for _, to, way in work:
            copy_of, inward, outward = (down_copy, down_in, down_out) if way else (up_copy, up_in, up_out)
            comes = here < chips - 1 if way else here > 0
            if to == here:
                if not filled:
                    total[...] = both(here)
                    filled = True
                copy_of(to).wait_recv()
                total[...] += inward[to].astype(jnp.float32)
            else:
                partial = both(to)
                if comes:
                    copy_of(to).wait_recv()
                    partial = partial + inward[to].astype(jnp.float32)
                outward[to] = partial.astype(jnp.bfloat16)
                started.append(copy_of(to))
                started[-1].start()
        for copy in started:
            copy.wait_send()

    for here in range(chips):
        pl.when(chip == here)(functools.partial(at_chip, here))


def merge(chips, packed):
    rows, channels = packed.shape
    owned = rows // (2 * chips)
    dma = pltpu.SemaphoreType.DMA
    line = 2 <= chips <= 4
    block = pltpu.VMEM((chips, owned, channels), jnp.bfloat16)
    return pl.pallas_call(
        functools.partial(line_kernel if line else merge_kernel, chips),
        out_shape=jax.ShapeDtypeStruct((owned, channels), jnp.float32),
        in_specs=[pl.BlockSpec(memory_space=pl.ANY)],
        out_specs=pl.BlockSpec(memory_space=pltpu.VMEM),
        scratch_shapes=[block] * (6 if line else 4) + [dma((chips,))] * (7 if line else 5),
        compiler_params=pltpu.CompilerParams(
            collective_id=1, has_side_effects=True, vmem_limit_bytes=60 * 1024 * 1024
        ),
        name="merge",
    )(packed)


def local(sections, replicas, token_ids, embed, weights, variance, momentum, worker_error, server_error, cotangent):
    width, channels = weights.shape[2:]
    owned = 2 * width // replicas
    chips = replicas // 2
    left, right, shared = run_blocks(sections, chips, token_ids, embed, weights, cotangent, momentum[0])
    packed, new_worker = pack(
        left.reshape(2, -1, width),
        right.reshape(2, -1, channels),
        shared,
        worker_error.reshape(2 * width, channels),
    )
    total = merge(chips, packed)
    merged = total / replicas + server_error[0]
    server_scale = jnp.sqrt(jnp.mean(merged * merged) + 0.01)
    server_values = (server_scale * jnp.tanh(merged / server_scale)).astype(jnp.bfloat16)
    new_server = (merged - server_values.astype(jnp.float32))[None]
    start = lax.axis_index("dp") * owned
    own_weights = lax.dynamic_slice_in_dim(weights[0].reshape(2 * width, channels), start, owned, 0)
    step_size = (
        0.01 * server_values.astype(jnp.float32) / (jnp.sqrt(variance[0].astype(jnp.float32)) + 1e-08)
    )
    new_weights = (own_weights.astype(jnp.float32) - step_size).astype(jnp.bfloat16)[None]
    return (new_weights, server_values[None], new_worker.reshape(worker_error.shape), new_server)


def solution(mesh):
    in_specs = (
        P(None, "dp"),
        P(),
        P("section", None, None, None),
        P("section", "dp", None),
        P("section", "dp", None),
        P("section", "dp", None, None, None),
        P("section", "dp", None),
        P(None, "dp", None),
    )
    out_specs = (
        P("section", "dp", None),
        P("section", "dp", None),
        P("section", "dp", None, None, None),
        P("section", "dp", None),
    )
    body = functools.partial(local, mesh.shape["section"], mesh.shape["dp"])
    return jax.shard_map(body, mesh=mesh, in_specs=in_specs, out_specs=out_specs, check_vma=False)
```

```python
import functools
import math

import jax
import jax.numpy as jnp
from jax import lax
from jax.experimental import pallas as pl
from jax.experimental.pallas import tpu as pltpu
from jax.sharding import PartitionSpec as P

gelu_coef = math.sqrt(2.0 / math.pi)
MESH = pl.DeviceIdType.MESH
NT = (((1,), (1,)), ((), ()))
TN = (((0,), (0,)), ((), ()))


def dot(left, right, dims=(((1,), (0,)), ((), ()))):
    return lax.dot_general(left, right, dims, preferred_element_type=jnp.float32)


def dp_device(index):
    return {"section": lax.axis_index("section"), "dp": index}


def section_device(index):
    return {"section": index, "dp": lax.axis_index("dp")}


def signal(semaphore, device):
    pl.semaphore_signal(semaphore, inc=1, device_id=device, device_id_type=MESH)


def remote(src, dst, send, recv, device):
    return pltpu.make_async_remote_copy(
        src_ref=src, dst_ref=dst, send_sem=send, recv_sem=recv, device_id=device, device_id_type=MESH
    )


def block_kernel(
    sections, chips, ids, embed_in, weights_in, cotangent_in, momentum, left, right, shared,
    embed, first_matrix, second_matrix, cotangent, load_sem, arrived, outgoing, back_arrived, back_outgoing, normed_s, scaled_s, slope_s,
    fwd_send, fwd_recv, bwd_send, bwd_recv, own_sem, up_send, up_recv, down_send, down_recv, pair_send, pair_recv,
):
    micro, rows, width = cotangent.shape
    vocab = embed.shape[0]
    channels = first_matrix.shape[-1]
    loads = [
        pltpu.make_async_copy(embed_in, embed, load_sem.at[0]),
        pltpu.make_async_copy(weights_in.at[0, 0], first_matrix, load_sem.at[1]),
        pltpu.make_async_copy(weights_in.at[0, 1], second_matrix, load_sem.at[2]),
        pltpu.make_async_copy(cotangent_in, cotangent, load_sem.at[3]),
    ]
    for load in loads:
        load.start()
    tile = min(512, channels)
    owned = momentum.shape[0]
    section = lax.axis_index("section")
    me = lax.axis_index("dp")
    chip, core = me // 2, me % 2
    partner = chip * 2 + 1 - core
    first, last = section == 0, section == sections - 1
    ahead, behind = lax.rem(section + 1, sections), lax.rem(section + sections - 1, sections)

    barrier = pltpu.get_barrier_semaphore()
    signal(barrier, section_device(ahead))
    signal(barrier, section_device(behind))
    signal(barrier, dp_device(partner))
    for j in range(1, chips):
        signal(barrier, dp_device(lax.rem(chip + j, chips) * 2 + core))
    pl.semaphore_wait(barrier, 2 + chips)

    def span(index):
        return pl.ds(pl.multiple_of(index * owned, owned), owned)

    own_copy = pltpu.make_async_copy(momentum, shared.at[span(me)], own_sem)
    own_copy.start()

    def up_copy(hop):
        rows_of = span(me - 2 * hop)
        source = momentum if hop == 0 else shared.at[rows_of]
        return remote(source, shared.at[rows_of], up_send.at[hop], up_recv.at[hop], dp_device(me + 2))

    def down_copy(hop):
        rows_of = span(me + 2 * hop)
        source = momentum if hop == 0 else shared.at[rows_of]
        return remote(source, shared.at[rows_of], down_send.at[hop], down_recv.at[hop], dp_device(me - 2))

    def pair_copy(slot, index):
        source = momentum if slot == 0 else shared.at[span(index)]
        return remote(source, shared.at[span(index)], pair_send.at[slot], pair_recv.at[slot], dp_device(partner))

    def pass_on(hop):
        if hop > 0:
            @pl.when(chip >= hop)
            def _():
                up_copy(hop - 1).wait_recv()

        @pl.when(jnp.logical_and(chip >= hop, chip < chips - 1))
        def _():
            up_copy(hop).start()

        if hop > 0:
            @pl.when(chip + hop < chips)
            def _():
                down_copy(hop - 1).wait_recv()

        @pl.when(jnp.logical_and(chip + hop < chips, chip > 0))
        def _():
            down_copy(hop).start()

        if hop == 0:
            pair_copy(0, me).start()
        else:
            @pl.when(chip >= hop)
            def _():
                pair_copy(2 * hop - 1, me - 2 * hop).start()

            @pl.when(chip + hop < chips)
            def _():
                pair_copy(2 * hop, me + 2 * hop).start()

    pass_on(0)

    def fwd_copy(m):
        return remote(outgoing.at[m], arrived.at[m], fwd_send.at[m], fwd_recv.at[m], section_device(ahead))

    def bwd_copy(m):
        return remote(
            back_outgoing.at[m], back_arrived.at[m], bwd_send.at[m], bwd_recv.at[m], section_device(behind)
        )

    loads[0].wait()

    @pl.when(first)
    def _():
        for m in range(micro):
            hot = ids[m : m + 1, :] == lax.broadcasted_iota(jnp.int32, (vocab, rows), 0)
            hot = jnp.where(hot, 1.0, 0.0).astype(jnp.bfloat16)
            arrived[m] = dot(hot, embed[...], TN).astype(jnp.bfloat16)

    loads[1].wait()
    if chips > 2:
        @pl.when(last)
        def _():
            pass_on(1)

    def forward(m, carry):
        @pl.when(jnp.logical_not(first))
        def _():
            fwd_copy(m).wait_recv()

        values = arrived[m].astype(jnp.float32)
        center = jnp.mean(values, axis=-1, keepdims=True)
        shifted = values - center
        spread = jnp.mean(shifted * shifted, axis=-1, keepdims=True)
        scaled = lax.rsqrt(spread + 1e-05)
        normed = shifted * scaled
        normed_b = normed.astype(jnp.bfloat16)
        normed_s[m] = normed
        scaled_s[m] = scaled
        left[0, m] = normed_b
        mixed = values
        for start in range(0, channels, tile):
            cut = slice(start, start + tile)
            upper = dot(normed_b, first_matrix[:, cut])
            square = upper * upper
            bent = jnp.tanh(gelu_coef * (upper + 0.044715 * upper * square))
            half = 0.5 * (1.0 + bent)
            hidden = (upper * half).astype(jnp.bfloat16)
            right[1, m, :, cut] = hidden
            slope_s[m, :, cut] = half + 0.5 * upper * (1.0 - bent * bent) * gelu_coef * (
                1.0 + 3.0 * 0.044715 * square
            )

        @pl.when(m == 0)
        def _():
            loads[2].wait()

        for start in range(0, channels, tile):
            cut = slice(start, start + tile)
            mixed = mixed + dot(right[1, m, :, cut], second_matrix[:, cut], NT)
        outgoing[m] = mixed.astype(jnp.bfloat16)

        @pl.when(jnp.logical_not(last))
        def _():
            fwd_copy(m).start()

        return carry

    lax.fori_loop(0, micro, forward, 0)
    loads[3].wait()

    @pl.when(jnp.logical_not(last))
    def _():
        for hop in range(1, chips - 1):
            pass_on(hop)

    def backward(m, carry):
        @pl.when(last)
        def _():
            left[1, m] = cotangent[m]

        @pl.when(jnp.logical_not(last))
        def _():
            bwd_copy(m).wait_recv()
            left[1, m] = back_arrived[m]

        grad_out = left[1, m]
        for start in range(0, channels, tile):
            cut = slice(start, start + tile)
            back_hidden = dot(grad_out, second_matrix[:, cut])
            back_upper = (back_hidden * slope_s[m, :, cut]).astype(jnp.bfloat16)
            right[0, m, :, cut] = back_upper

        @pl.when(jnp.logical_not(first))
        def _():
            back_normed = jnp.zeros((rows, width), jnp.float32)
            for start in range(0, channels, tile):
                cut = slice(start, start + tile)
                back_normed = back_normed + dot(right[0, m, :, cut], first_matrix[:, cut], NT)
            normed = normed_s[m]
            first_mean = jnp.mean(back_normed, axis=-1, keepdims=True)
            second_mean = jnp.mean(back_normed * normed, axis=-1, keepdims=True)
            back_outgoing[m] = (
                grad_out.astype(jnp.float32) + scaled_s[m] * (back_normed - first_mean - normed * second_mean)
            ).astype(jnp.bfloat16)
            bwd_copy(m).start()

        return carry

    lax.fori_loop(0, micro, backward, 0)

    @pl.when(last)
    def _():
        for hop in range(2, chips - 1):
            pass_on(hop)

    pass_on(chips - 1)
    own_copy.wait()
    pair_copy(0, me).wait()
    for hop in range(chips):
        @pl.when(jnp.logical_and(chip >= hop, chip < chips - 1))
        def _():
            up_copy(hop).wait_send()

        @pl.when(jnp.logical_and(chip + hop < chips, chip > 0))
        def _():
            down_copy(hop).wait_send()

        if hop > 0:
            @pl.when(chip >= hop)
            def _():
                pair_copy(2 * hop - 1, me - 2 * hop).wait()

            @pl.when(chip + hop < chips)
            def _():
                pair_copy(2 * hop, me + 2 * hop).wait()

    @pl.when(jnp.logical_not(last))
    def _():
        for m in range(micro):
            fwd_copy(m).wait_send()

    @pl.when(jnp.logical_not(first))
    def _():
        for m in range(micro):
            bwd_copy(m).wait_send()


def run_blocks(sections, chips, ids, embed, weights, cotangent, momentum):
    micro, rows, width = cotangent.shape
    channels = weights.shape[-1]
    vmem = pl.BlockSpec(memory_space=pltpu.VMEM)
    hbm = pl.BlockSpec(memory_space=pl.ANY)
    relay = pltpu.VMEM((micro, rows, width), jnp.bfloat16)
    dma = pltpu.SemaphoreType.DMA
    return pl.pallas_call(
        functools.partial(block_kernel, sections, chips),
        out_shape=(
            jax.ShapeDtypeStruct((2, micro, rows, width), jnp.bfloat16),
            jax.ShapeDtypeStruct((2, micro, rows, channels), jnp.bfloat16),
            jax.ShapeDtypeStruct((2 * width, channels), jnp.bfloat16),
        ),
        in_specs=[vmem, hbm, hbm, hbm, hbm],
        out_specs=(vmem, vmem, hbm),
        scratch_shapes=[
            pltpu.VMEM(embed.shape, jnp.bfloat16),
            pltpu.VMEM((width, channels), jnp.bfloat16),
            pltpu.VMEM((width, channels), jnp.bfloat16),
            relay, dma((4,)), relay, relay, relay, relay,
            pltpu.VMEM((micro, rows, width), jnp.float32),
            pltpu.VMEM((micro, rows, 1), jnp.float32),
            pltpu.VMEM((micro, rows, channels), jnp.float32),
            dma((micro,)), dma((micro,)), dma((micro,)), dma((micro,)),
            dma, dma((chips,)), dma((chips,)), dma((chips,)), dma((chips,)),
            dma((2 * chips,)), dma((2 * chips,)),
        ],
        compiler_params=pltpu.CompilerParams(
            collective_id=0, has_side_effects=True, vmem_limit_bytes=60 * 1024 * 1024
        ),
        name="blocks",
    )(ids, embed, weights, cotangent, momentum)


def pack_kernel(count, left, right, shared, error, packed, fresh, combined, total):
    phase, step = pl.program_id(0), pl.program_id(1)

    @pl.when(jnp.logical_and(phase == 0, step == 0))
    def _():
        total[...] = jnp.zeros_like(total)

    @pl.when(phase == 0)
    def _():
        gradient = dot(left[0], right[0], TN)
        values = 0.9 * shared[...].astype(jnp.float32) + 0.1 * gradient + error[...].astype(jnp.float32)
        combined[step] = values
        total[...] += jnp.sum(values * values, axis=0, keepdims=True)

    @pl.when(phase == 1)
    def _():
        mean = jnp.sum(total[...], axis=1, keepdims=True) / count
        scale = jnp.sqrt(mean + 0.01)
        values = combined[step]
        narrow = (scale * jnp.tanh(values * (1.0 / scale))).astype(jnp.bfloat16)
        packed[...] = narrow
        fresh[...] = (values - narrow.astype(jnp.float32)).astype(jnp.bfloat16)


def pack(left, right, shared, error):
    _, tokens, width = left.shape
    channels = right.shape[-1]
    tile = 128
    per = width // tile
    steps = 2 * per

    def when_first(phase, step):
        return jnp.where(phase == 0, step, steps - 1)

    rows_in = pl.BlockSpec((tile, channels), lambda p, i: (when_first(p, i), 0))
    rows_out = pl.BlockSpec((tile, channels), lambda p, i: (jnp.where(p == 0, 0, i), 0))
    out = jax.ShapeDtypeStruct((2 * width, channels), jnp.bfloat16)
    return pl.pallas_call(
        functools.partial(pack_kernel, float(2 * width * channels)),
        grid=(2, steps),
        out_shape=(out, out),
        in_specs=[
            pl.BlockSpec((1, tokens, tile), lambda p, i: (when_first(p, i) // per, 0, when_first(p, i) % per)),
            pl.BlockSpec((1, tokens, channels), lambda p, i: (when_first(p, i) // per, 0, 0)),
            rows_in,
            rows_in,
        ],
        out_specs=(rows_out, rows_out),
        scratch_shapes=[
            pltpu.VMEM((steps, tile, channels), jnp.float32),
            pltpu.VMEM((1, channels), jnp.float32),
        ],
        compiler_params=pltpu.CompilerParams(
            dimension_semantics=("arbitrary", "arbitrary"), vmem_limit_bytes=60 * 1024 * 1024
        ),
        name="pack",
    )(left, right, shared, error)


def merge_kernel(
    chips, packed, total, own, paired, outgoing, arrived,
    own_sem, pair_send, pair_recv, far_send, far_recv,
):
    owned = total.shape[0]
    me = lax.axis_index("dp")
    chip, core = me // 2, me % 2
    other = 1 - core
    partner = chip * 2 + other

    barrier = pltpu.get_barrier_semaphore()
    signal(barrier, dp_device(partner))
    for j in range(1, chips):
        signal(barrier, dp_device(lax.rem(chip + j, chips) * 2 + core))
    pl.semaphore_wait(barrier, chips)

    def span(index):
        return pl.ds(pl.multiple_of(index * owned, owned), owned)

    order = list(range(1, chips)) + [0]
    local, pair, far = {}, {}, {}
    for j in order:
        target = lax.rem(chip + j, chips) * 2
        pair[j] = remote(
            packed.at[span(target + other)], paired.at[j], pair_send.at[j], pair_recv.at[j], dp_device(partner)
        )
        pair[j].start()
        local[j] = pltpu.make_async_copy(packed.at[span(target + core)], own.at[j], own_sem.at[j])
        local[j].start()
    for j in order:
        local[j].wait()
        pair[j].wait()
        both = own[j].astype(jnp.float32) + paired[j].astype(jnp.float32)
        if j == 0:
            total[...] = both
        else:
            outgoing[j - 1] = both.astype(jnp.bfloat16)
            target = lax.rem(chip + j, chips) * 2 + core
            far[j] = remote(
                outgoing.at[j - 1], arrived.at[j - 1], far_send.at[j], far_recv.at[j], dp_device(target)
            )
            far[j].start()
    for j in range(1, chips):
        far[j].wait()
        total[...] += arrived[j - 1].astype(jnp.float32)


def line_kernel(
    chips, packed, total, own, paired, up_out, up_in, down_out, down_in,
    own_sem, pair_send, pair_recv, up_send, up_recv, down_send, down_recv,
):
    owned = total.shape[0]
    me = lax.axis_index("dp")
    chip, core = me // 2, me % 2
    other = 1 - core
    partner = chip * 2 + other

    barrier = pltpu.get_barrier_semaphore()
    signal(barrier, dp_device(partner))
    for j in range(1, chips):
        signal(barrier, dp_device(lax.rem(chip + j, chips) * 2 + core))
    pl.semaphore_wait(barrier, chips)

    def span(index):
        return pl.ds(pl.multiple_of(index * owned, owned), owned)

    def up_copy(to):
        return remote(up_out.at[to], up_in.at[to], up_send.at[to], up_recv.at[to], dp_device(me + 2))

    def down_copy(to):
        return remote(down_out.at[to], down_in.at[to], down_send.at[to], down_recv.at[to], dp_device(me - 2))

    def at_chip(here):
        work = [(here + chips - 1 - to, to, 0) for to in range(here, chips) if to > here or here > 0]
        work += [(chips - 1 - here + to, to, 1) for to in range(here + 1) if to < here or here < chips - 1]
        work.sort()
        order = []
        for _, to, _ in work:
            if to != here and to not in order:
                order.append(to)
        order.append(here)
        local, pair, done, started = {}, {}, set(), []
        for to in order:
            pair[to] = remote(
                packed.at[span(2 * to + other)], paired.at[to], pair_send.at[to], pair_recv.at[to], dp_device(partner)
            )
            pair[to].start()
            local[to] = pltpu.make_async_copy(packed.at[span(2 * to + core)], own.at[to], own_sem.at[to])
            local[to].start()

        def both(to):
            if to not in done:
                done.add(to)
                local[to].wait()
                pair[to].wait()
            return own[to].astype(jnp.float32) + paired[to].astype(jnp.float32)

        filled = False
        for _, to, way in work:
            copy_of, inward, outward = (down_copy, down_in, down_out) if way else (up_copy, up_in, up_out)
            comes = here < chips - 1 if way else here > 0
            if to == here:
                if not filled:
                    total[...] = both(here)
                    filled = True
                copy_of(to).wait_recv()
                total[...] += inward[to].astype(jnp.float32)
            else:
                partial = both(to)
                if comes:
                    copy_of(to).wait_recv()
                    partial = partial + inward[to].astype(jnp.float32)
                outward[to] = partial.astype(jnp.bfloat16)
                started.append(copy_of(to))
                started[-1].start()
        for copy in started:
            copy.wait_send()

    for here in range(chips):
        pl.when(chip == here)(functools.partial(at_chip, here))


def merge(chips, packed):
    rows, channels = packed.shape
    owned = rows // (2 * chips)
    dma = pltpu.SemaphoreType.DMA
    line = 2 <= chips <= 4
    block = pltpu.VMEM((chips, owned, channels), jnp.bfloat16)
    return pl.pallas_call(
        functools.partial(line_kernel if line else merge_kernel, chips),
        out_shape=jax.ShapeDtypeStruct((owned, channels), jnp.float32),
        in_specs=[pl.BlockSpec(memory_space=pl.ANY)],
        out_specs=pl.BlockSpec(memory_space=pltpu.VMEM),
        scratch_shapes=[block] * (6 if line else 4) + [dma((chips,))] * (7 if line else 5),
        compiler_params=pltpu.CompilerParams(
            collective_id=1, has_side_effects=True, vmem_limit_bytes=60 * 1024 * 1024
        ),
        name="merge",
    )(packed)


def update_kernel(
    replicas, total_in, error_in, weights_in, variance_in, new_weights, new_momentum, new_error,
    total, error, weights, variance, sems,
):
    owned = new_weights.shape[1]
    start = lax.axis_index("dp") * owned
    rows = pl.ds(pl.multiple_of(start, owned), owned)
    loads = [
        pltpu.make_async_copy(total_in, total, sems.at[0]),
        pltpu.make_async_copy(error_in.at[0], error, sems.at[1]),
        pltpu.make_async_copy(weights_in.at[rows], weights, sems.at[2]),
        pltpu.make_async_copy(variance_in.at[0], variance, sems.at[3]),
    ]
    for load in loads:
        load.start()
    loads[0].wait()
    loads[1].wait()
    merged = total[...] / replicas + error[...]
    mean = jnp.sum(jnp.sum(merged * merged, axis=0, keepdims=True), axis=1, keepdims=True) / merged.size
    scale = jnp.sqrt(mean + 0.01)
    total[...] = merged
    values = (scale * jnp.tanh(merged * (1.0 / scale))).astype(jnp.bfloat16)
    new_momentum[0] = values
    wide = values.astype(jnp.float32)
    new_error[0] = total[...] - wide
    loads[2].wait()
    loads[3].wait()
    step_size = 0.01 * wide / (jnp.sqrt(variance[...].astype(jnp.float32)) + 1e-08)
    new_weights[0] = (weights[...].astype(jnp.float32) - step_size).astype(jnp.bfloat16)


def update(replicas, total, server_error, weights, variance):
    hbm = pl.BlockSpec(memory_space=pl.ANY)
    vmem = pl.BlockSpec(memory_space=pltpu.VMEM)
    narrow = jax.ShapeDtypeStruct(variance.shape, jnp.bfloat16)
    return pl.pallas_call(
        functools.partial(update_kernel, replicas),
        out_shape=(narrow, narrow, jax.ShapeDtypeStruct(variance.shape, jnp.float32)),
        in_specs=[hbm] * 4,
        out_specs=(vmem, vmem, vmem),
        scratch_shapes=[
            pltpu.VMEM(total.shape, jnp.float32),
            pltpu.VMEM(total.shape, jnp.float32),
            pltpu.VMEM(total.shape, jnp.bfloat16),
            pltpu.VMEM(total.shape, jnp.bfloat16),
            pltpu.SemaphoreType.DMA((4,)),
        ],
        compiler_params=pltpu.CompilerParams(vmem_limit_bytes=60 * 1024 * 1024),
        name="update",
    )(total, server_error, weights, variance)


def local(sections, replicas, token_ids, embed, weights, variance, momentum, worker_error, server_error, cotangent):
    width, channels = weights.shape[2:]
    chips = replicas // 2
    left, right, shared = run_blocks(sections, chips, token_ids, embed, weights, cotangent, momentum[0])
    packed, new_worker = pack(
        left.reshape(2, -1, width),
        right.reshape(2, -1, channels),
        shared,
        worker_error.reshape(2 * width, channels),
    )
    total = merge(chips, packed)
    new_weights, new_momentum, new_server = update(
        replicas, total, server_error, weights.reshape(2 * width, channels), variance
    )
    return (new_weights, new_momentum, new_worker.reshape(worker_error.shape), new_server)


def solution(mesh):
    in_specs = (
        P(None, "dp"),
        P(),
        P("section", None, None, None),
        P("section", "dp", None),
        P("section", "dp", None),
        P("section", "dp", None, None, None),
        P("section", "dp", None),
        P(None, "dp", None),
    )
    out_specs = (
        P("section", "dp", None),
        P("section", "dp", None),
        P("section", "dp", None, None, None),
        P("section", "dp", None),
    )
    body = functools.partial(local, mesh.shape["section"], mesh.shape["dp"])
    return jax.shard_map(body, mesh=mesh, in_specs=in_specs, out_specs=out_specs, check_vma=False)
```

```python
import functools
import math

import jax
import jax.numpy as jnp
from jax import lax
from jax.experimental import pallas as pl
from jax.experimental.pallas import tpu as pltpu
from jax.sharding import PartitionSpec as P

gelu_coef = math.sqrt(2.0 / math.pi)
MESH = pl.DeviceIdType.MESH
NT = (((1,), (1,)), ((), ()))
TN = (((0,), (0,)), ((), ()))


def dot(left, right, dims=(((1,), (0,)), ((), ()))):
    return lax.dot_general(left, right, dims, preferred_element_type=jnp.float32)


def dp_device(index):
    return {"section": lax.axis_index("section"), "dp": index}


def section_device(index):
    return {"section": index, "dp": lax.axis_index("dp")}


def signal(semaphore, device):
    pl.semaphore_signal(semaphore, inc=1, device_id=device, device_id_type=MESH)


def remote(src, dst, send, recv, device):
    return pltpu.make_async_remote_copy(
        src_ref=src, dst_ref=dst, send_sem=send, recv_sem=recv, device_id=device, device_id_type=MESH
    )


def block_kernel(
    sections, chips, ids, embed_in, weights_in, cotangent_in, momentum, left, right, shared,
    embed, first_matrix, second_matrix, cotangent, load_sem, arrived, outgoing, back_arrived, back_outgoing, normed_s, scaled_s, slope_s,
    fwd_send, fwd_recv, bwd_send, bwd_recv, own_sem, up_send, up_recv, down_send, down_recv, pair_send, pair_recv,
):
    micro, rows, width = cotangent.shape
    vocab = embed.shape[0]
    channels = first_matrix.shape[-1]
    loads = [
        pltpu.make_async_copy(embed_in, embed, load_sem.at[0]),
        pltpu.make_async_copy(weights_in.at[0, 0], first_matrix, load_sem.at[1]),
        pltpu.make_async_copy(weights_in.at[0, 1], second_matrix, load_sem.at[2]),
        pltpu.make_async_copy(cotangent_in, cotangent, load_sem.at[3]),
    ]
    for load in loads:
        load.start()
    tile = min(512, channels)
    owned = momentum.shape[0]
    section = lax.axis_index("section")
    me = lax.axis_index("dp")
    chip, core = me // 2, me % 2
    partner = chip * 2 + 1 - core
    first, last = section == 0, section == sections - 1
    ahead, behind = lax.rem(section + 1, sections), lax.rem(section + sections - 1, sections)

    barrier = pltpu.get_barrier_semaphore()
    signal(barrier, section_device(ahead))
    signal(barrier, section_device(behind))
    signal(barrier, dp_device(partner))
    for j in range(1, chips):
        signal(barrier, dp_device(lax.rem(chip + j, chips) * 2 + core))
    pl.semaphore_wait(barrier, 2 + chips)

    def span(index):
        return pl.ds(pl.multiple_of(index * owned, owned), owned)

    own_copy = pltpu.make_async_copy(momentum, shared.at[span(me)], own_sem)
    own_copy.start()

    def up_copy(hop):
        rows_of = span(me - 2 * hop)
        source = momentum if hop == 0 else shared.at[rows_of]
        return remote(source, shared.at[rows_of], up_send.at[hop], up_recv.at[hop], dp_device(me + 2))

    def down_copy(hop):
        rows_of = span(me + 2 * hop)
        source = momentum if hop == 0 else shared.at[rows_of]
        return remote(source, shared.at[rows_of], down_send.at[hop], down_recv.at[hop], dp_device(me - 2))

    def pair_copy(slot, index):
        source = momentum if slot == 0 else shared.at[span(index)]
        return remote(source, shared.at[span(index)], pair_send.at[slot], pair_recv.at[slot], dp_device(partner))

    def pass_on(hop):
        if hop > 0:
            @pl.when(chip >= hop)
            def _():
                up_copy(hop - 1).wait_recv()

        @pl.when(jnp.logical_and(chip >= hop, chip < chips - 1))
        def _():
            up_copy(hop).start()

        if hop > 0:
            @pl.when(chip + hop < chips)
            def _():
                down_copy(hop - 1).wait_recv()

        @pl.when(jnp.logical_and(chip + hop < chips, chip > 0))
        def _():
            down_copy(hop).start()

        if hop == 0:
            pair_copy(0, me).start()
        else:
            @pl.when(chip >= hop)
            def _():
                pair_copy(2 * hop - 1, me - 2 * hop).start()

            @pl.when(chip + hop < chips)
            def _():
                pair_copy(2 * hop, me + 2 * hop).start()

    pass_on(0)

    def fwd_copy(m):
        return remote(outgoing.at[m], arrived.at[m], fwd_send.at[m], fwd_recv.at[m], section_device(ahead))

    def bwd_copy(m):
        return remote(
            back_outgoing.at[m], back_arrived.at[m], bwd_send.at[m], bwd_recv.at[m], section_device(behind)
        )

    loads[0].wait()

    @pl.when(first)
    def _():
        for m in range(micro):
            hot = ids[m : m + 1, :] == lax.broadcasted_iota(jnp.int32, (vocab, rows), 0)
            hot = jnp.where(hot, 1.0, 0.0).astype(jnp.bfloat16)
            arrived[m] = dot(hot, embed[...], TN).astype(jnp.bfloat16)

    loads[1].wait()
    if chips > 2:
        @pl.when(last)
        def _():
            pass_on(1)

    def forward(m, carry):
        @pl.when(jnp.logical_not(first))
        def _():
            fwd_copy(m).wait_recv()

        values = arrived[m].astype(jnp.float32)
        center = jnp.mean(values, axis=-1, keepdims=True)
        shifted = values - center
        spread = jnp.mean(shifted * shifted, axis=-1, keepdims=True)
        scaled = lax.rsqrt(spread + 1e-05)
        normed = shifted * scaled
        normed_b = normed.astype(jnp.bfloat16)
        normed_s[m] = normed
        scaled_s[m] = scaled
        left[0, m] = normed_b
        mixed = values
        for start in range(0, channels, tile):
            cut = slice(start, start + tile)
            upper = dot(normed_b, first_matrix[:, cut])
            square = upper * upper
            bent = jnp.tanh(gelu_coef * (upper + 0.044715 * upper * square))
            half = 0.5 * (1.0 + bent)
            hidden = (upper * half).astype(jnp.bfloat16)
            right[1, m, :, cut] = hidden
            slope_s[m, :, cut] = half + 0.5 * upper * (1.0 - bent * bent) * gelu_coef * (
                1.0 + 3.0 * 0.044715 * square
            )

        @pl.when(m == 0)
        def _():
            loads[2].wait()

        for start in range(0, channels, tile):
            cut = slice(start, start + tile)
            mixed = mixed + dot(right[1, m, :, cut], second_matrix[:, cut], NT)
        outgoing[m] = mixed.astype(jnp.bfloat16)

        @pl.when(jnp.logical_not(last))
        def _():
            fwd_copy(m).start()

        return carry

    lax.fori_loop(0, micro, forward, 0)
    loads[3].wait()

    @pl.when(jnp.logical_not(last))
    def _():
        for hop in range(1, chips - 1):
            pass_on(hop)

    def backward(m, carry):
        @pl.when(last)
        def _():
            left[1, m] = cotangent[m]

        @pl.when(jnp.logical_not(last))
        def _():
            bwd_copy(m).wait_recv()
            left[1, m] = back_arrived[m]

        grad_out = left[1, m]
        for start in range(0, channels, tile):
            cut = slice(start, start + tile)
            back_hidden = dot(grad_out, second_matrix[:, cut])
            back_upper = (back_hidden * slope_s[m, :, cut]).astype(jnp.bfloat16)
            right[0, m, :, cut] = back_upper

        @pl.when(jnp.logical_not(first))
        def _():
            back_normed = jnp.zeros((rows, width), jnp.float32)
            for start in range(0, channels, tile):
                cut = slice(start, start + tile)
                back_normed = back_normed + dot(right[0, m, :, cut], first_matrix[:, cut], NT)
            normed = normed_s[m]
            first_mean = jnp.mean(back_normed, axis=-1, keepdims=True)
            second_mean = jnp.mean(back_normed * normed, axis=-1, keepdims=True)
            back_outgoing[m] = (
                grad_out.astype(jnp.float32) + scaled_s[m] * (back_normed - first_mean - normed * second_mean)
            ).astype(jnp.bfloat16)
            bwd_copy(m).start()

        return carry

    lax.fori_loop(0, micro, backward, 0)

    @pl.when(last)
    def _():
        for hop in range(2, chips - 1):
            pass_on(hop)

    pass_on(chips - 1)
    own_copy.wait()
    pair_copy(0, me).wait()
    for hop in range(chips):
        @pl.when(jnp.logical_and(chip >= hop, chip < chips - 1))
        def _():
            up_copy(hop).wait_send()

        @pl.when(jnp.logical_and(chip + hop < chips, chip > 0))
        def _():
            down_copy(hop).wait_send()

        if hop > 0:
            @pl.when(chip >= hop)
            def _():
                pair_copy(2 * hop - 1, me - 2 * hop).wait()

            @pl.when(chip + hop < chips)
            def _():
                pair_copy(2 * hop, me + 2 * hop).wait()

    @pl.when(jnp.logical_not(last))
    def _():
        for m in range(micro):
            fwd_copy(m).wait_send()

    @pl.when(jnp.logical_not(first))
    def _():
        for m in range(micro):
            bwd_copy(m).wait_send()


def run_blocks(sections, chips, ids, embed, weights, cotangent, momentum):
    micro, rows, width = cotangent.shape
    channels = weights.shape[-1]
    vmem = pl.BlockSpec(memory_space=pltpu.VMEM)
    hbm = pl.BlockSpec(memory_space=pl.ANY)
    relay = pltpu.VMEM((micro, rows, width), jnp.bfloat16)
    dma = pltpu.SemaphoreType.DMA
    return pl.pallas_call(
        functools.partial(block_kernel, sections, chips),
        out_shape=(
            jax.ShapeDtypeStruct((2, micro, rows, width), jnp.bfloat16),
            jax.ShapeDtypeStruct((2, micro, rows, channels), jnp.bfloat16),
            jax.ShapeDtypeStruct((2 * width, channels), jnp.bfloat16),
        ),
        in_specs=[vmem, hbm, hbm, hbm, hbm],
        out_specs=(vmem, vmem, hbm),
        scratch_shapes=[
            pltpu.VMEM(embed.shape, jnp.bfloat16),
            pltpu.VMEM((width, channels), jnp.bfloat16),
            pltpu.VMEM((width, channels), jnp.bfloat16),
            relay, dma((4,)), relay, relay, relay, relay,
            pltpu.VMEM((micro, rows, width), jnp.float32),
            pltpu.VMEM((micro, rows, 1), jnp.float32),
            pltpu.VMEM((micro, rows, channels), jnp.float32),
            dma((micro,)), dma((micro,)), dma((micro,)), dma((micro,)),
            dma, dma((chips,)), dma((chips,)), dma((chips,)), dma((chips,)),
            dma((2 * chips,)), dma((2 * chips,)),
        ],
        compiler_params=pltpu.CompilerParams(
            collective_id=0, has_side_effects=True, vmem_limit_bytes=60 * 1024 * 1024
        ),
        name="blocks",
    )(ids, embed, weights, cotangent, momentum)


def pack_kernel(count, left, right, shared, error, packed, fresh, combined, total):
    phase, step = pl.program_id(0), pl.program_id(1)

    @pl.when(jnp.logical_and(phase == 0, step == 0))
    def _():
        total[...] = jnp.zeros_like(total)

    @pl.when(phase == 0)
    def _():
        gradient = dot(left[0], right[0], TN)
        values = 0.9 * shared[...].astype(jnp.float32) + 0.1 * gradient + error[...].astype(jnp.float32)
        combined[step] = values
        total[...] += jnp.sum(values * values, axis=0, keepdims=True)

    @pl.when(phase == 1)
    def _():
        mean = jnp.sum(total[...], axis=1, keepdims=True) / count
        scale = jnp.sqrt(mean + 0.01)
        values = combined[step]
        narrow = (scale * jnp.tanh(values * (1.0 / scale))).astype(jnp.bfloat16)
        packed[...] = narrow
        fresh[...] = (values - narrow.astype(jnp.float32)).astype(jnp.bfloat16)


def pack(left, right, shared, error):
    _, tokens, width = left.shape
    channels = right.shape[-1]
    tile = min(256, width)
    per = width // tile
    steps = 2 * per

    def when_first(phase, step):
        return jnp.where(phase == 0, step, steps - 1)

    rows_in = pl.BlockSpec((tile, channels), lambda p, i: (when_first(p, i), 0))
    rows_out = pl.BlockSpec((tile, channels), lambda p, i: (jnp.where(p == 0, 0, i), 0))
    out = jax.ShapeDtypeStruct((2 * width, channels), jnp.bfloat16)
    return pl.pallas_call(
        functools.partial(pack_kernel, float(2 * width * channels)),
        grid=(2, steps),
        out_shape=(out, out),
        in_specs=[
            pl.BlockSpec((1, tokens, tile), lambda p, i: (when_first(p, i) // per, 0, when_first(p, i) % per)),
            pl.BlockSpec((1, tokens, channels), lambda p, i: (when_first(p, i) // per, 0, 0)),
            rows_in,
            rows_in,
        ],
        out_specs=(rows_out, rows_out),
        scratch_shapes=[
            pltpu.VMEM((steps, tile, channels), jnp.float32),
            pltpu.VMEM((1, channels), jnp.float32),
        ],
        compiler_params=pltpu.CompilerParams(
            dimension_semantics=("arbitrary", "arbitrary"), vmem_limit_bytes=60 * 1024 * 1024
        ),
        name="pack",
    )(left, right, shared, error)


def merge_kernel(
    chips, packed, total, own, paired, outgoing, arrived,
    own_sem, pair_send, pair_recv, far_send, far_recv,
):
    owned = total.shape[0]
    me = lax.axis_index("dp")
    chip, core = me // 2, me % 2
    other = 1 - core
    partner = chip * 2 + other

    barrier = pltpu.get_barrier_semaphore()
    signal(barrier, dp_device(partner))
    for j in range(1, chips):
        signal(barrier, dp_device(lax.rem(chip + j, chips) * 2 + core))
    pl.semaphore_wait(barrier, chips)

    def span(index):
        return pl.ds(pl.multiple_of(index * owned, owned), owned)

    order = list(range(1, chips)) + [0]
    local, pair, far = {}, {}, {}
    for j in order:
        target = lax.rem(chip + j, chips) * 2
        pair[j] = remote(
            packed.at[span(target + other)], paired.at[j], pair_send.at[j], pair_recv.at[j], dp_device(partner)
        )
        pair[j].start()
        local[j] = pltpu.make_async_copy(packed.at[span(target + core)], own.at[j], own_sem.at[j])
        local[j].start()
    for j in order:
        local[j].wait()
        pair[j].wait()
        both = own[j].astype(jnp.float32) + paired[j].astype(jnp.float32)
        if j == 0:
            total[...] = both
        else:
            outgoing[j - 1] = both.astype(jnp.bfloat16)
            target = lax.rem(chip + j, chips) * 2 + core
            far[j] = remote(
                outgoing.at[j - 1], arrived.at[j - 1], far_send.at[j], far_recv.at[j], dp_device(target)
            )
            far[j].start()
    for j in range(1, chips):
        far[j].wait()
        total[...] += arrived[j - 1].astype(jnp.float32)


def line_kernel(
    chips, packed, total, own, paired, up_out, up_in, down_out, down_in,
    own_sem, pair_send, pair_recv, up_send, up_recv, down_send, down_recv,
):
    owned = total.shape[0]
    me = lax.axis_index("dp")
    chip, core = me // 2, me % 2
    other = 1 - core
    partner = chip * 2 + other

    def span(index):
        return pl.ds(pl.multiple_of(index * owned, owned), owned)

    def own_copy(to):
        return pltpu.make_async_copy(packed.at[span(2 * to + core)], own.at[to], own_sem.at[to])

    for to in range(chips):
        own_copy(to).start()

    barrier = pltpu.get_barrier_semaphore()
    signal(barrier, dp_device(partner))
    for j in range(1, chips):
        signal(barrier, dp_device(lax.rem(chip + j, chips) * 2 + core))
    pl.semaphore_wait(barrier, chips)

    def up_copy(to):
        return remote(up_out.at[to], up_in.at[to], up_send.at[to], up_recv.at[to], dp_device(me + 2))

    def down_copy(to):
        return remote(down_out.at[to], down_in.at[to], down_send.at[to], down_recv.at[to], dp_device(me - 2))

    def at_chip(here):
        work = [(here + chips - 1 - to, to, 0) for to in range(here, chips) if to > here or here > 0]
        work += [(chips - 1 - here + to, to, 1) for to in range(here + 1) if to < here or here < chips - 1]
        work.sort()
        order = []
        for _, to, _ in work:
            if to != here and to not in order:
                order.append(to)
        order.append(here)
        pair, done, started = {}, set(), []
        for to in order:
            pair[to] = remote(
                packed.at[span(2 * to + other)], paired.at[to], pair_send.at[to], pair_recv.at[to], dp_device(partner)
            )
            pair[to].start()

        def both(to):
            if to not in done:
                done.add(to)
                own_copy(to).wait()
                pair[to].wait()
            return own[to].astype(jnp.float32) + paired[to].astype(jnp.float32)

        filled = False
        for _, to, way in work:
            copy_of, inward, outward = (down_copy, down_in, down_out) if way else (up_copy, up_in, up_out)
            comes = here < chips - 1 if way else here > 0
            if to == here:
                if not filled:
                    total[...] = both(here)
                    filled = True
                copy_of(to).wait_recv()
                total[...] += inward[to].astype(jnp.float32)
            else:
                partial = both(to)
                if comes:
                    copy_of(to).wait_recv()
                    partial = partial + inward[to].astype(jnp.float32)
                outward[to] = partial.astype(jnp.bfloat16)
                started.append(copy_of(to))
                started[-1].start()
        for copy in started:
            copy.wait_send()

    for here in range(chips):
        pl.when(chip == here)(functools.partial(at_chip, here))


def merge(chips, packed):
    rows, channels = packed.shape
    owned = rows // (2 * chips)
    dma = pltpu.SemaphoreType.DMA
    line = 2 <= chips <= 4
    block = pltpu.VMEM((chips, owned, channels), jnp.bfloat16)
    return pl.pallas_call(
        functools.partial(line_kernel if line else merge_kernel, chips),
        out_shape=jax.ShapeDtypeStruct((owned, channels), jnp.float32),
        in_specs=[pl.BlockSpec(memory_space=pl.ANY)],
        out_specs=pl.BlockSpec(memory_space=pltpu.VMEM),
        scratch_shapes=[block] * (6 if line else 4) + [dma((chips,))] * (7 if line else 5),
        compiler_params=pltpu.CompilerParams(
            collective_id=1, has_side_effects=True, vmem_limit_bytes=60 * 1024 * 1024
        ),
        name="merge",
    )(packed)


def update_kernel(
    replicas, total_in, error_in, weights_in, variance_in, new_weights, new_momentum, new_error,
    total, error, weights, variance, sems,
):
    owned = new_weights.shape[1]
    start = lax.axis_index("dp") * owned
    rows = pl.ds(pl.multiple_of(start, owned), owned)
    loads = [
        pltpu.make_async_copy(total_in, total, sems.at[0]),
        pltpu.make_async_copy(error_in.at[0], error, sems.at[1]),
        pltpu.make_async_copy(weights_in.at[rows], weights, sems.at[2]),
        pltpu.make_async_copy(variance_in.at[0], variance, sems.at[3]),
    ]
    for load in loads:
        load.start()
    loads[0].wait()
    loads[1].wait()
    merged = total[...] / replicas + error[...]
    mean = jnp.sum(jnp.sum(merged * merged, axis=0, keepdims=True), axis=1, keepdims=True) / merged.size
    scale = jnp.sqrt(mean + 0.01)
    total[...] = merged
    values = (scale * jnp.tanh(merged * (1.0 / scale))).astype(jnp.bfloat16)
    new_momentum[0] = values
    wide = values.astype(jnp.float32)
    new_error[0] = total[...] - wide
    loads[2].wait()
    loads[3].wait()
    step_size = 0.01 * wide / (jnp.sqrt(variance[...].astype(jnp.float32)) + 1e-08)
    new_weights[0] = (weights[...].astype(jnp.float32) - step_size).astype(jnp.bfloat16)


def update(replicas, total, server_error, weights, variance):
    hbm = pl.BlockSpec(memory_space=pl.ANY)
    vmem = pl.BlockSpec(memory_space=pltpu.VMEM)
    narrow = jax.ShapeDtypeStruct(variance.shape, jnp.bfloat16)
    return pl.pallas_call(
        functools.partial(update_kernel, replicas),
        out_shape=(narrow, narrow, jax.ShapeDtypeStruct(variance.shape, jnp.float32)),
        in_specs=[hbm] * 4,
        out_specs=(vmem, vmem, vmem),
        scratch_shapes=[
            pltpu.VMEM(total.shape, jnp.float32),
            pltpu.VMEM(total.shape, jnp.float32),
            pltpu.VMEM(total.shape, jnp.bfloat16),
            pltpu.VMEM(total.shape, jnp.bfloat16),
            pltpu.SemaphoreType.DMA((4,)),
        ],
        compiler_params=pltpu.CompilerParams(vmem_limit_bytes=60 * 1024 * 1024),
        name="update",
    )(total, server_error, weights, variance)


def local(sections, replicas, token_ids, embed, weights, variance, momentum, worker_error, server_error, cotangent):
    width, channels = weights.shape[2:]
    chips = replicas // 2
    left, right, shared = run_blocks(sections, chips, token_ids, embed, weights, cotangent, momentum[0])
    packed, new_worker = pack(
        left.reshape(2, -1, width),
        right.reshape(2, -1, channels),
        shared,
        worker_error.reshape(2 * width, channels),
    )
    total = merge(chips, packed)
    new_weights, new_momentum, new_server = update(
        replicas, total, server_error, weights.reshape(2 * width, channels), variance
    )
    return (new_weights, new_momentum, new_worker.reshape(worker_error.shape), new_server)


def solution(mesh):
    in_specs = (
        P(None, "dp"),
        P(),
        P("section", None, None, None),
        P("section", "dp", None),
        P("section", "dp", None),
        P("section", "dp", None, None, None),
        P("section", "dp", None),
        P(None, "dp", None),
    )
    out_specs = (
        P("section", "dp", None),
        P("section", "dp", None),
        P("section", "dp", None, None, None),
        P("section", "dp", None),
    )
    body = functools.partial(local, mesh.shape["section"], mesh.shape["dp"])
    return jax.shard_map(body, mesh=mesh, in_specs=in_specs, out_specs=out_specs, check_vma=False)
```
